32 devices in a mesh: band: 4 (over x, core), grid: 8 (over z, y).
Axes of the slice: x: 2, y: 2, z: 4, core: 2. Of those that a mesh axis runs over, the one named last changes fastest.
Arguments:
- orbitals: float32 [8, 128, 128, 128], P('band', 'grid'), may hold values from -6 to 6
- occupation: float32 [8], P('band'), may hold values from 0.25 to 1
- g_list: int32 [131072], P('grid'), may hold values from 0 to 262143, as said below
- positions: float32 [3, 512], replicated, may hold values from 0 to 1
- species: int32 [512], replicated, may hold values from 0 to 3
- widths: float32 [4], replicated, may hold values from 0.3 to 2
Outputs:
- stress: float32 [3, 3], replicated
- atom_terms: float32 [512], replicated
The draws below stay inside these ranges and needn't reach their ends.
Inputs may be any that keep to these rules, and one draw needn't show every extreme that they name: `g_list`: within each aligned block of 16384 entries the values are distinct and increasing.
All inputs are finite; a program needn't handle non-finite values.
Results may differ from the reference program's by a relative error of at most 0.00013.
Values sent between devices are 32-bit elements; how exact they have to be, the bound alone decides.
No kernel may reach another device: no remote copies, remote signals or barrier semaphores. Data moves between devices by JAX's collectives and lax.ppermute only.
A program may use at most 64 MiB of HBM per device.

```python
import math
import jax
import jax.numpy as jnp
from jax import lax

NX = 128
NY = 128
NZ = 128
GSEL_DEV = 16384
ATOMS = 512
SPECIES = 4
NBANDS = 8
SLAB_Y = 16
N_GRID = 8


def draw_orbitals(key, part):
    key_noise = jax.random.fold_in(key, 11)
    key_amplitude = jax.random.fold_in(key, 12)
    key_modes = jax.random.fold_in(key, 13)
    key_offset = jax.random.fold_in(key, 14)
    key_filter = jax.random.fold_in(key, 16)
    key_envelope = jax.random.fold_in(key, 17)
    shape = (NBANDS, NX, NY, NZ)
    noise_part = 0.3 * jnp.clip(jax.random.normal(key_noise, shape, jnp.float32), -4.0, 4.0)
    strength = jax.random.uniform(key_filter, (NBANDS,), jnp.float32, 0.04, 0.12)
    swing = jax.random.uniform(jax.random.fold_in(key_envelope, 1), (NBANDS,), jnp.float32, 0.1, 0.3)
    amp_low = 0.3
    amp_high = 0.55
    beside = jnp.roll(noise_part, 1, axis=1) + jnp.roll(noise_part, -1, axis=1)
    beside = beside + jnp.roll(noise_part, 1, axis=2) + jnp.roll(noise_part, -1, axis=2)
    beside = beside + jnp.roll(noise_part, 1, axis=3) + jnp.roll(noise_part, -1, axis=3)
    colored = noise_part + strength[:, None, None, None] * beside
    axis_x = jnp.arange(NX, dtype=jnp.float32)[None, :, None, None] / NX
    axis_y = jnp.arange(NY, dtype=jnp.float32)[None, None, :, None] / NY
    axis_z = jnp.arange(NZ, dtype=jnp.float32)[None, None, None, :] / NZ
    low_x = jax.random.randint(jax.random.fold_in(key_envelope, 2), (NBANDS,), -2, 3).astype(jnp.float32)
    low_y = jax.random.randint(jax.random.fold_in(key_envelope, 3), (NBANDS,), -2, 3).astype(jnp.float32)
    low_z = jax.random.randint(jax.random.fold_in(key_envelope, 4), (NBANDS,), -2, 3).astype(jnp.float32)
    low_phase = jax.random.uniform(jax.random.fold_in(key_envelope, 5), (NBANDS,), jnp.float32, -math.pi, math.pi)
    envelope_angle = 2.0 * math.pi * (low_x[:, None, None, None] * axis_x + low_y[:, None, None, None] * axis_y + low_z[:, None, None, None] * axis_z) + low_phase[:, None, None, None]
    envelope = 1.0 + swing[:, None, None, None] * jnp.cos(envelope_angle)
    start = (envelope * colored).astype(jnp.float32)

    def add_wave(wave, result):
        wave_key = jax.random.fold_in(key_modes, wave)
        mode_x = jax.random.randint(jax.random.fold_in(wave_key, 1), (NBANDS,), -(NX // 2), NX // 2).astype(jnp.float32)
        mode_y = jax.random.randint(jax.random.fold_in(wave_key, 2), (NBANDS,), -(NY // 2), NY // 2).astype(jnp.float32)
        mode_z = jax.random.randint(jax.random.fold_in(wave_key, 3), (NBANDS,), -(NZ // 2), NZ // 2).astype(jnp.float32)
        offset = jax.random.uniform(jax.random.fold_in(key_offset, wave), (NBANDS,), jnp.float32, -math.pi, math.pi)
        amplitude = jax.random.uniform(jax.random.fold_in(key_amplitude, wave), (NBANDS,), jnp.float32, amp_low, amp_high)
        angles = 2.0 * math.pi * (mode_x[:, None, None, None] * axis_x + mode_y[:, None, None, None] * axis_y + mode_z[:, None, None, None] * axis_z) + offset[:, None, None, None]
        return result + amplitude[:, None, None, None] * jnp.cos(angles)
    result = lax.fori_loop(0, 48, add_wave, start)
    return jnp.clip(result, -6.0, 6.0)


def draw_g_list(key, part):
    local_cells = NX * SLAB_Y * NZ
    slab_keys = jax.random.split(jax.random.fold_in(key, 21), N_GRID)

    def one_slab(slab_key):
        return jnp.sort(jax.random.permutation(slab_key, local_cells)[:GSEL_DEV])
    return jax.vmap(one_slab)(slab_keys).reshape(-1).astype(jnp.int32)


def touch_ends(values, stream_key, smallest, largest):
    longest = values.shape.index(max(values.shape))
    spots = []
    for shift in (0, 1):
        where = [jax.random.randint(jax.random.fold_in(stream_key, axis), (), 0, length) for axis, length in enumerate(values.shape)]
        where[longest] = (where[longest] + shift) % values.shape[longest]
        spots.append(tuple(where))
    return values.at[spots[0]].set(smallest).at[spots[1]].set(largest)


def shard_levels(key, extent, pieces, low, high):
    gain, own = 1.0, jax.random.fold_in(key, 6)
    for position, blocks in pieces:
        steps = jnp.exp(jax.random.uniform(jax.random.fold_in(own, position), (blocks,), jnp.float32, low / len(pieces), high / len(pieces)))
        gain = gain * jnp.repeat(steps, extent[position] // blocks).reshape([-1 if axis == position else 1 for axis in range(len(extent))])
    return gain


def setup_inputs(seed: int = 0) -> dict:
    splits = jax.random.split(jax.random.key(seed), 7)
    return {
        "orbitals": draw_orbitals(jax.random.fold_in(splits[6], 71), 0),
        "occupation": jnp.clip(0.25 + 0.75 * jax.random.uniform(splits[1], (NBANDS,), jnp.float32) ** shard_levels(splits[1], (NBANDS,), ((0, 4),), -0.2, 0.2), 0.25, 1.0),
        "g_list": draw_g_list(jax.random.fold_in(splits[6], 71), 0),
        "positions": jnp.clip(jax.random.uniform(splits[3], (3, ATOMS), jnp.float32, 0.0, 1.0), 0.0, 1.0),
        "species": touch_ends(jax.random.randint(splits[4], (ATOMS,), 0, SPECIES), jax.random.fold_in(splits[4], 1), 0, SPECIES - 1).astype(jnp.int32),
        "widths": jnp.clip(jnp.exp(jax.random.uniform(splits[5], (SPECIES,), jnp.float32, math.log(0.3), math.log(2.0))), 0.3, 2.0),
    }


HIGHEST = lax.Precision.HIGHEST


def folded_frequency(cell, length):
    folded = jnp.where(cell < length // 2, cell, cell - length)
    return folded.astype(jnp.float32)


def spectrum_sums(selected, freq_x, freq_y, freq_z, positions, species, widths, lengths, band_total):
    two_pi = 2.0 * math.pi
    wave_vector = jnp.stack([two_pi * freq_x / lengths[0], two_pi * freq_y / lengths[1], two_pi * freq_z / lengths[2]])
    wave_square = jnp.sum(wave_vector * wave_vector, axis=0)
    nonzero = (wave_square > 0).astype(jnp.float32)
    denominator = wave_square + 1.0 - nonzero
    weighted = selected * (4.0 * math.pi) * nonzero / denominator
    identity = jnp.eye(3, dtype=jnp.float32)[:, :, None]
    kernel = 2.0 * wave_vector[:, None, :] * wave_vector[None, :, :] / denominator - identity
    stress = jnp.sum(kernel * weighted[None, None, :], axis=2) / band_total
    form_factor = jnp.exp(-0.5 * wave_square[None, :] * (widths * widths)[:, None]) * weighted[None, :]
    kinds = widths.shape[0]
    one_hot = (species[:, None] == jnp.arange(kinds, dtype=jnp.int32)[None, :]).astype(jnp.float32)
    atom_count = species.shape[0]
    fractions = positions.reshape(3, atom_count // 32, 32).transpose(1, 0, 2)
    hot_rows = one_hot.reshape(atom_count // 32, 32, kinds)

    def atom_block(operands):
        fraction, hot_block = operands
        phases = two_pi * (fraction[0][:, None] * freq_x[None, :] + fraction[1][:, None] * freq_y[None, :] + fraction[2][:, None] * freq_z[None, :])
        projected = jnp.dot(jnp.cos(phases), form_factor.T, precision=HIGHEST)
        return jnp.sum(projected * hot_block, axis=1)

    atom_terms = lax.map(atom_block, (fractions, hot_rows)).reshape(atom_count) / band_total
    return stress, atom_terms


def reference(orbitals, occupation, g_list, positions, species, widths):
    cells = NX * NY * NZ

    def add_band(accumulated, operands):
        orbital_row, occupied = operands
        pair_rows = orbital_row[None] * orbitals
        spectra = jnp.fft.fftn(pair_rows, axes=(1, 2, 3)) / cells
        pair_power = jnp.real(spectra) ** 2 + jnp.imag(spectra) ** 2
        weights = occupied * occupation
        return accumulated + jnp.einsum("p,pxyz->xyz", weights, pair_power, precision=HIGHEST), None

    spectrum, ignored = lax.scan(add_band, jnp.zeros((NX, NY, NZ), jnp.float32), (orbitals, occupation))
    entries = jnp.arange(g_list.shape[0], dtype=jnp.int32)
    slab_index = entries // GSEL_DEV
    cell_x = g_list // (SLAB_Y * NZ)
    cell_y = slab_index * SLAB_Y + (g_list // NZ) % SLAB_Y
    cell_z = g_list % NZ
    selected = spectrum[cell_x, cell_y, cell_z]
    return spectrum_sums(selected, folded_frequency(cell_x, NX), folded_frequency(cell_y, NY), folded_frequency(cell_z, NZ), positions, species, widths, (NX, NY, NZ), NBANDS)
```

```python
import functools
import math

import jax
import jax.numpy as jnp
from jax import lax
from jax.experimental import pallas as pl
from jax.experimental.pallas import tpu as pltpu
from jax.sharding import PartitionSpec as P

HIGH = lax.Precision.HIGH


def shifted(array, axis, by):
    peers = lax.axis_size(axis)
    return lax.ppermute(array, axis, [(i, (i + by) % peers) for i in range(peers)])


def dft_tables(length):
    indices = jnp.arange(length, dtype=jnp.int32)
    products = indices[:, None] * indices[None, :] % length
    angles = 2.0 * math.pi / length * products.astype(jnp.float32)
    return (jnp.cos(angles), jnp.sin(angles))


def folded(cell, length, nyquist_up):
    keep = cell <= length // 2 if nyquist_up else cell < length // 2
    return jnp.where(keep, cell, cell - length).astype(jnp.float32)


def mask_kernel(chunks, row_ref, col_ref, out_ref):
    step = pl.program_id(0)
    rows, cols = out_ref.shape[1:]
    width = row_ref.shape[-1]

    @pl.when((step == 0) | (step == chunks))
    def _():
        out_ref[...] = jnp.zeros_like(out_ref)

    one_row = lax.broadcasted_iota(jnp.int32, (rows, width), 0) == row_ref[0]
    one_col = lax.broadcasted_iota(jnp.int32, (cols, width), 0) == col_ref[0]
    out_ref[0] += lax.dot_general(
        one_row.astype(jnp.bfloat16),
        one_col.astype(jnp.bfloat16),
        (((1,), (1,)), ((), ())),
        preferred_element_type=jnp.float32,
    )


def entry_masks(row_ids, col_ids, rows, cols):
    entries = row_ids.shape[1]
    width = math.gcd(entries, 512)
    chunks = entries // width
    row_ids = row_ids.reshape(3 * chunks, 1, width)
    col_ids = col_ids.reshape(3 * chunks, 1, width)
    id_spec = pl.BlockSpec((1, 1, width), lambda i: (i, 0, 0))
    return pl.pallas_call(
        functools.partial(mask_kernel, chunks),
        grid=(3 * chunks,),
        in_specs=[id_spec, id_spec],
        out_specs=pl.BlockSpec((1, rows, cols), lambda i: (jnp.where(i < chunks, 0, 1), 0, 0)),
        out_shape=jax.ShapeDtypeStruct((2, rows, cols), jnp.float32),
        compiler_params=pltpu.CompilerParams(dimension_semantics=("arbitrary",)),
        cost_estimate=pl.CostEstimate(
            flops=12 * entries * rows * cols, bytes_accessed=2 * rows * cols * 4, transcendentals=0
        ),
        name="entry_masks",
    )(row_ids, col_ids)


def per_device(orbitals, occupation, g_list, positions, species, widths):
    block_bands, slab_x, size_y, size_z = orbitals.shape
    grid_count = lax.axis_size("grid")
    band_count = lax.axis_size("band")
    band_index = lax.axis_index("band")
    grid_index = lax.axis_index("grid")
    size_x = slab_x * grid_count
    slab_y = size_y // grid_count
    cells = size_x * size_y * size_z
    scale = 1.0 / float(cells)

    own = jnp.transpose(orbitals, (0, 2, 1, 3))
    others = {}
    for distance in range(1, band_count // 2 + 1):
        others[distance] = shifted((own, occupation), "band", distance)

    def split(code):
        return (
            code // (slab_y * size_z),
            code // size_z % slab_y,
            code % size_z,
        )

    mirror = lax.ppermute(
        g_list, "grid", [(d, grid_count - 1 - d) for d in range(grid_count)]
    )
    mirror_zero = lax.ppermute(
        g_list, "grid", [(d, (grid_count - d) % grid_count) for d in range(grid_count)]
    )
    own_x, own_y, own_z = split(g_list)
    mir_x, mir_y, mir_z = split(mirror)
    zer_x, zer_y, zer_z = split(mirror_zero)
    row_ids = jnp.stack(
        [
            own_y * size_x + own_x,
            jnp.where(mir_y > 0, (slab_y - mir_y) * size_x + (size_x - mir_x) % size_x, -1),
            jnp.where(zer_y == 0, (size_x - zer_x) % size_x, -1),
        ]
    )
    col_ids = jnp.stack([own_z, (size_z - mir_z) % size_z, (size_z - zer_z) % size_z])
    masks = entry_masks(row_ids, col_ids, slab_y * size_x, size_z)
    masks = masks.reshape(2, slab_y, size_x, size_z)

    cos_x, sin_x = dft_tables(size_x)
    cos_y, sin_y = dft_tables(size_y)
    cos_z, sin_z = dft_tables(size_z)
    z_real = jnp.concatenate([cos_z, sin_z], axis=0)
    z_imag = jnp.concatenate([-sin_z, cos_z], axis=0)
    y_real = jnp.stack([cos_y, sin_y], axis=1)
    y_imag = jnp.stack([-sin_y, cos_y], axis=1)
    y_matrix = jnp.stack([y_real, y_imag], axis=1).reshape(2 * size_y, 2 * size_y)
    cos_xs = cos_x.reshape(size_x, grid_count, slab_x)
    sin_xs = sin_x.reshape(size_x, grid_count, slab_x)
    x_real = jnp.stack([cos_xs, sin_xs], axis=2).reshape(size_x, 2 * size_x)
    x_imag = jnp.stack([-sin_xs, cos_xs], axis=2).reshape(size_x, 2 * size_x)

    pairs = []
    for a in range(block_bands):
        for b in range(a, block_bands):
            weight = occupation[a] * occupation[b] * (1.0 if a == b else 2.0)
            pairs.append((own[a], own[b], weight))
    pairs.sort(key=lambda pair: pair[0] is not pair[1])
    for distance in range(1, band_count // 2 + 1):
        there, there_occupied = others[distance]
        if 2 * distance < band_count:
            for a in range(block_bands):
                for b in range(block_bands):
                    pairs.append((own[a], there[b], 2.0 * occupation[a] * there_occupied[b]))
            continue
        for a in range(block_bands):
            for b in range(a + 1, block_bands):
                pairs.append((own[a], there[b], 2.0 * occupation[a] * there_occupied[b]))
        first = band_index < distance
        half = block_bands // 2
        for a in range(half):
            left = jnp.where(first, own[a], own[a + half])
            right = jnp.where(first, there[a], there[a + half])
            left_occupied = jnp.where(first, occupation[a], occupation[a + half])
            right_occupied = jnp.where(first, there_occupied[a], there_occupied[a + half])
            pairs.append((left, right, 2.0 * left_occupied * right_occupied))
        if block_bands % 2:
            last = block_bands - 1
            pairs.append((own[last], there[last], occupation[last] * there_occupied[last]))

    def density(pair):
        left, right, weight = pair
        return left * right * jnp.sqrt(weight)

    power = None
    for start in range(0, len(pairs), 2):
        first_density = density(pairs[start])
        if start + 1 < len(pairs):
            both = jnp.concatenate([first_density, density(pairs[start + 1])], axis=2)
            along_z = jnp.stack(
                [
                    jnp.einsum("yxz,zk->yxk", both, z_real, precision=HIGH),
                    jnp.einsum("yxz,zk->yxk", both, z_imag, precision=HIGH),
                ]
            )
        else:
            along_z = jnp.stack(
                [
                    jnp.einsum("yxz,zk->yxk", first_density, cos_z, precision=HIGH),
                    jnp.einsum("yxz,zk->yxk", first_density, -sin_z, precision=HIGH),
                ]
            )
        along_z = along_z.reshape(2 * size_y, slab_x, size_z)
        along_y = jnp.einsum("qp,pxk->qxk", y_matrix, along_z, precision=HIGH)
        received = lax.all_to_all(along_y, "grid", split_axis=0, concat_axis=0, tiled=True)
        received = received.reshape(grid_count, slab_y, 2, slab_x, size_z)
        lines = jnp.transpose(received, (1, 0, 2, 3, 4)).reshape(slab_y, 2 * size_x, size_z)
        real_part = jnp.einsum("np,rpk->rnk", x_real, lines, precision=HIGH)
        imag_part = jnp.einsum("np,rpk->rnk", x_imag, lines, precision=HIGH)
        pack_power = real_part * real_part + imag_part * imag_part
        power = pack_power if power is None else power + pack_power

    two_pi = 2.0 * math.pi
    kinds = widths.shape[0]
    one_hot = species[:, None] == jnp.arange(kinds, dtype=jnp.int32)[None, :]
    atom_width = jnp.sum(jnp.where(one_hot, widths[None, :], 0.0), axis=1)
    cell_x = jnp.arange(size_x, dtype=jnp.int32)
    cell_y = grid_index * slab_y + jnp.arange(slab_y, dtype=jnp.int32)
    cell_z = jnp.arange(size_z, dtype=jnp.int32)

    def factors(freq, length, fraction):
        wave = two_pi * freq / length
        turns = freq[:, None] * fraction[None, :]
        angles = two_pi * (turns - jnp.round(turns))
        damping = jnp.exp(-0.5 * (wave * wave)[:, None] * (atom_width * atom_width)[None, :])
        return damping * jnp.cos(angles), damping * jnp.sin(angles)

    stress = jnp.zeros((3, 3), jnp.float32)
    atom_terms = jnp.zeros(species.shape, jnp.float32)
    for which, nyquist_up in ((0, False), (1, True)):
        freq_x = folded(cell_x, size_x, nyquist_up)
        freq_y = folded(cell_y, size_y, nyquist_up)
        freq_z = folded(cell_z, size_z, nyquist_up)
        wave_x = (two_pi * freq_x / size_x)[None, :, None]
        wave_y = (two_pi * freq_y / size_y)[:, None, None]
        wave_z = (two_pi * freq_z / size_z)[None, None, :]
        wave_square = wave_x * wave_x + wave_y * wave_y + wave_z * wave_z
        nonzero = (wave_square > 0).astype(jnp.float32)
        denominator = wave_square + 1.0 - nonzero
        kept = masks[which] * (0.5 * scale * scale * 4.0 * math.pi) * nonzero / denominator
        weighted = power * kept
        along = weighted * 2.0 / denominator
        total = jnp.sum(weighted)
        waves = (wave_x, wave_y, wave_z)
        entries = {}
        for a in range(3):
            for b in range(a, 3):
                entries[a, b] = jnp.sum(along * waves[a] * waves[b])
        stress = stress + jnp.stack(
            [
                jnp.stack([entries[min(a, b), max(a, b)] for b in range(3)])
                for a in range(3)
            ]
        ) - total * jnp.eye(3, dtype=jnp.float32)
        xr, xi = factors(freq_x, size_x, positions[0])
        yr, yi = factors(freq_y, size_y, positions[1])
        zr, zi = factors(freq_z, size_z, positions[2])
        tr = jnp.einsum("rnk,kj->rnj", weighted, zr, precision=HIGH)
        ti = jnp.einsum("rnk,kj->rnj", weighted, zi, precision=HIGH)
        ur = jnp.sum(xr[None] * tr - xi[None] * ti, axis=1)
        ui = jnp.sum(xr[None] * ti + xi[None] * tr, axis=1)
        atom_terms = atom_terms + jnp.sum(yr * ur - yi * ui, axis=0)

    packed = jnp.concatenate([stress.reshape(-1), atom_terms]) / (block_bands * band_count)
    packed = lax.psum(packed, ("band", "grid"))
    return (packed[:9].reshape(3, 3), packed[9:])


def solution(mesh):
    return jax.shard_map(
        per_device,
        mesh=mesh,
        in_specs=(P("band", "grid", None, None), P("band"), P("grid"), P(), P(), P()),
        out_specs=(P(), P()),
        check_vma=False,
    )
```

```python
import functools
import math

import jax
import jax.numpy as jnp
from jax import lax
from jax.experimental import pallas as pl
from jax.experimental.pallas import tpu as pltpu
from jax.sharding import PartitionSpec as P

HIGH = lax.Precision.HIGH
HIGHEST = lax.Precision.HIGHEST


def shifted(array, axis, by):
    peers = lax.axis_size(axis)
    return lax.ppermute(array, axis, [(i, (i + by) % peers) for i in range(peers)])


def dft_tables(length):
    indices = jnp.arange(length, dtype=jnp.int32)
    products = indices[:, None] * indices[None, :] % length
    angles = 2.0 * math.pi / length * products.astype(jnp.float32)
    return (jnp.cos(angles), jnp.sin(angles))


def folded(cell, length, nyquist_up):
    keep = cell <= length // 2 if nyquist_up else cell < length // 2
    return jnp.where(keep, cell, cell - length).astype(jnp.float32)


def mask_kernel(row_ref, col_ref, out_ref):
    rows, cols = out_ref.shape
    width = row_ref.shape[-1]

    @pl.when(pl.program_id(0) == 0)
    def _():
        out_ref[...] = jnp.zeros_like(out_ref)

    one_row = lax.broadcasted_iota(jnp.int32, (rows, width), 0) == row_ref[0]
    one_col = lax.broadcasted_iota(jnp.int32, (cols, width), 0) == col_ref[0]
    out_ref[...] += lax.dot_general(
        one_row.astype(jnp.bfloat16),
        one_col.astype(jnp.bfloat16),
        (((1,), (1,)), ((), ())),
        preferred_element_type=jnp.float32,
    )


def entry_mask(row_ids, col_ids, rows, cols):
    entries = row_ids.shape[0]
    width = math.gcd(entries, 512)
    chunks = entries // width
    id_spec = pl.BlockSpec((1, 1, width), lambda i: (i, 0, 0))
    return pl.pallas_call(
        mask_kernel,
        grid=(chunks,),
        in_specs=[id_spec, id_spec],
        out_specs=pl.BlockSpec((rows, cols), lambda i: (0, 0)),
        out_shape=jax.ShapeDtypeStruct((rows, cols), jnp.float32),
        compiler_params=pltpu.CompilerParams(dimension_semantics=("arbitrary",)),
        cost_estimate=pl.CostEstimate(
            flops=4 * entries * rows * cols, bytes_accessed=rows * cols * 4, transcendentals=0
        ),
        name="entry_mask",
    )(row_ids.reshape(chunks, 1, width), col_ids.reshape(chunks, 1, width))


def per_device(orbitals, occupation, g_list, positions, species, widths):
    block_bands, slab_x, size_y, size_z = orbitals.shape
    grid_count = lax.axis_size("grid")
    band_count = lax.axis_size("band")
    band_index = lax.axis_index("band")
    grid_index = lax.axis_index("grid")
    size_x = slab_x * grid_count
    slab_y = size_y // grid_count
    cells = size_x * size_y * size_z
    scale = 1.0 / float(cells)

    own = jnp.transpose(orbitals, (0, 2, 1, 3))
    others = {}
    for distance in range(1, band_count // 2 + 1):
        others[distance] = shifted((own, occupation), "band", distance)

    def split(code):
        return (
            code // (slab_y * size_z),
            code // size_z % slab_y,
            code % size_z,
        )

    mirror = lax.ppermute(
        g_list, "grid", [(d, grid_count - 1 - d) for d in range(grid_count)]
    )
    mirror_zero = lax.ppermute(
        g_list, "grid", [(d, (grid_count - d) % grid_count) for d in range(grid_count)]
    )
    own_x, own_y, own_z = split(g_list)
    mir_x, mir_y, mir_z = split(mirror)
    zer_x, zer_y, zer_z = split(mirror_zero)
    lists = [
        (own_y * size_x + own_x, own_z),
        (
            jnp.where(mir_y > 0, (slab_y - mir_y) * size_x + (size_x - mir_x) % size_x, -1),
            (size_z - mir_z) % size_z,
        ),
        (jnp.where(zer_y == 0, (size_x - zer_x) % size_x, -1), (size_z - zer_z) % size_z),
    ]

    cos_x, sin_x = dft_tables(size_x)
    cos_y, sin_y = dft_tables(size_y)
    cos_z, sin_z = dft_tables(size_z)
    z_real = jnp.concatenate([cos_z, sin_z], axis=0)
    z_imag = jnp.concatenate([-sin_z, cos_z], axis=0)
    y_real = jnp.stack([cos_y, sin_y], axis=1)
    y_imag = jnp.stack([-sin_y, cos_y], axis=1)
    y_matrix = jnp.stack([y_real, y_imag], axis=1).reshape(2 * size_y, 2 * size_y)
    cos_xs = cos_x.reshape(size_x, grid_count, slab_x)
    sin_xs = sin_x.reshape(size_x, grid_count, slab_x)
    x_real = jnp.stack([cos_xs, sin_xs], axis=2).reshape(size_x, 2 * size_x)
    x_imag = jnp.stack([-sin_xs, cos_xs], axis=2).reshape(size_x, 2 * size_x)

    pairs = []
    for a in range(block_bands):
        for b in range(a, block_bands):
            weight = occupation[a] * occupation[b] * (1.0 if a == b else 2.0)
            pairs.append((own[a], own[b], weight))
    pairs.sort(key=lambda pair: pair[0] is not pair[1])
    for distance in range(1, band_count // 2 + 1):
        there, there_occupied = others[distance]
        if 2 * distance < band_count:
            for a in range(block_bands):
                for b in range(block_bands):
                    pairs.append((own[a], there[b], 2.0 * occupation[a] * there_occupied[b]))
            continue
        for a in range(block_bands):
            for b in range(a + 1, block_bands):
                pairs.append((own[a], there[b], 2.0 * occupation[a] * there_occupied[b]))
        first = band_index < distance
        half = block_bands // 2
        for a in range(half):
            left = jnp.where(first, own[a], own[a + half])
            right = jnp.where(first, there[a], there[a + half])
            left_occupied = jnp.where(first, occupation[a], occupation[a + half])
            right_occupied = jnp.where(first, there_occupied[a], there_occupied[a + half])
            pairs.append((left, right, 2.0 * left_occupied * right_occupied))
        if block_bands % 2:
            last = block_bands - 1
            pairs.append((own[last], there[last], occupation[last] * there_occupied[last]))

    def density(pair):
        left, right, weight = pair
        return left * right * jnp.sqrt(weight)

    def finish(received):
        received = received.reshape(grid_count, slab_y, 2, slab_x, size_z)
        lines = jnp.transpose(received, (1, 0, 2, 3, 4)).reshape(slab_y, 2 * size_x, size_z)
        real_part = jnp.einsum("np,rpk->rnk", x_real, lines, precision=HIGH)
        imag_part = jnp.einsum("np,rpk->rnk", x_imag, lines, precision=HIGH)
        return real_part * real_part + imag_part * imag_part

    received = []
    power = None
    masks = []
    packs = [pairs[start : start + 2] for start in range(0, len(pairs), 2)]

    def add_power(power, arrived):
        pack_power = finish(arrived)
        return pack_power if power is None else power + pack_power

    along_y = None
    for pack, used in enumerate(packs):
        precision = HIGHEST if pack else HIGH
        if pack >= 2:
            power = add_power(power, received[pack - 2])
        if 1 <= pack <= 3:
            ids, _ = lax.optimization_barrier((lists[pack - 1], along_y))
            masks.append(entry_mask(*ids, slab_y * size_x, size_z))
        if pack:
            used, power, masks, _ = lax.optimization_barrier((used, power, masks, along_y))
        first_density = density(used[0])
        if len(used) > 1:
            both = jnp.concatenate([first_density, density(used[1])], axis=2)
            along_z = jnp.stack(
                [
                    jnp.einsum("yxz,zk->yxk", both, z_real, precision=precision),
                    jnp.einsum("yxz,zk->yxk", both, z_imag, precision=precision),
                ]
            )
        else:
            along_z = jnp.stack(
                [
                    jnp.einsum("yxz,zk->yxk", first_density, cos_z, precision=precision),
                    jnp.einsum("yxz,zk->yxk", first_density, -sin_z, precision=precision),
                ]
            )
        along_z = along_z.reshape(2 * size_y, slab_x, size_z)
        along_y = jnp.einsum("qp,pxk->qxk", y_matrix, along_z, precision=precision)
        if received:
            along_y, received[-1] = lax.optimization_barrier((along_y, received[-1]))
        received.append(
            lax.all_to_all(along_y, "grid", split_axis=0, concat_axis=0, tiled=True)
        )
    while len(masks) < 3:
        masks.append(entry_mask(*lists[len(masks)], slab_y * size_x, size_z))
    for arrived in received[max(len(packs) - 2, 0) :]:
        power = add_power(power, arrived)
    shape = (slab_y, size_x, size_z)
    masks = [masks[0].reshape(shape), (masks[1] + masks[2]).reshape(shape)]

    two_pi = 2.0 * math.pi
    kinds = widths.shape[0]
    one_hot = species[:, None] == jnp.arange(kinds, dtype=jnp.int32)[None, :]
    atom_width = jnp.sum(jnp.where(one_hot, widths[None, :], 0.0), axis=1)
    cell_x = jnp.arange(size_x, dtype=jnp.int32)
    cell_y = grid_index * slab_y + jnp.arange(slab_y, dtype=jnp.int32)
    cell_z = jnp.arange(size_z, dtype=jnp.int32)

    def factors(freq, length, fraction):
        wave = two_pi * freq / length
        turns = freq[:, None] * fraction[None, :]
        angles = two_pi * (turns - jnp.round(turns))
        damping = jnp.exp(-0.5 * (wave * wave)[:, None] * (atom_width * atom_width)[None, :])
        return damping * jnp.cos(angles), damping * jnp.sin(angles)

    moments = [0.0] * 7
    atom_terms = jnp.zeros(species.shape, jnp.float32)
    for which, nyquist_up in ((0, False), (1, True)):
        freq_x = folded(cell_x, size_x, nyquist_up)
        freq_y = folded(cell_y, size_y, nyquist_up)
        freq_z = folded(cell_z, size_z, nyquist_up)
        wave_x = (two_pi * freq_x / size_x)[None, :, None]
        wave_y = (two_pi * freq_y / size_y)[:, None, None]
        wave_z = (two_pi * freq_z / size_z)[None, None, :]
        wave_square = wave_x * wave_x + wave_y * wave_y + wave_z * wave_z
        nonzero = (wave_square > 0).astype(jnp.float32)
        denominator = wave_square + 1.0 - nonzero
        kept = masks[which] * (0.5 * scale * scale * 4.0 * math.pi) * nonzero / denominator
        weighted = power * kept
        along = weighted * 2.0 / denominator
        waves = (wave_x, wave_y, wave_z)
        terms = [along * waves[a] * waves[b] for a in range(3) for b in range(a, 3)]
        terms.append(weighted)
        moments = [moment + term for moment, term in zip(moments, terms)]
        xr, xi = factors(freq_x, size_x, positions[0])
        yr, yi = factors(freq_y, size_y, positions[1])
        zr, zi = factors(freq_z, size_z, positions[2])
        tr = jnp.einsum("rnk,kj->rnj", weighted, zr, precision=HIGH)
        ti = jnp.einsum("rnk,kj->rnj", weighted, zi, precision=HIGH)
        ur = jnp.sum(xr[None] * tr - xi[None] * ti, axis=1)
        ui = jnp.sum(xr[None] * ti + xi[None] * tr, axis=1)
        atom_terms = atom_terms + jnp.sum(yr * ur - yi * ui, axis=0)

    lanes = jnp.stack([jnp.sum(moment, axis=(0, 1)) for moment in moments])
    places = jnp.array([0, 1, 2, 1, 3, 4, 2, 4, 5], dtype=jnp.int32)[:, None]
    chosen = (places == jnp.arange(7, dtype=jnp.int32)[None, :]).astype(jnp.float32)
    diagonal = (jnp.arange(9, dtype=jnp.int32) % 4 == 0).astype(jnp.float32)
    last = (jnp.arange(7, dtype=jnp.int32) == 6).astype(jnp.float32)
    chosen = chosen - diagonal[:, None] * last[None, :]
    stress = jnp.sum(chosen[:, :, None] * lanes[None], axis=(1, 2))
    packed = jnp.concatenate([stress, atom_terms]) / (block_bands * band_count)
    packed = lax.psum(lax.psum(packed, "band"), "grid")
    return (packed[:9].reshape(3, 3), packed[9:])


def solution(mesh):
    return jax.shard_map(
        per_device,
        mesh=mesh,
        in_specs=(P("band", "grid", None, None), P("band"), P("grid"), P(), P(), P()),
        out_specs=(P(), P()),
        check_vma=False,
    )
```
